32 devices in a mesh: dp: 8 (over z, x), mp: 4 (over y, core).
Axes of the slice: x: 2, y: 2, z: 4, core: 2. Of those that a mesh axis runs over, the one named last changes fastest.
Arguments:
- tokens_in: bfloat16 [12288, 768], P(('dp', 'mp')), may hold values from -6 to 6
- skip_tokens: bfloat16 [12288, 768], P(('dp', 'mp')), may hold values from -6 to 6
- caption_flag: int32 [32], P('dp'), may hold values 0 or 1
- caption_mask: int32 [32, 77], P('dp'), may hold values 0 or 1
- w_skip: bfloat16 [1536, 768], P('dp', 'mp'), may hold values from -0.15625 to 0.15625
- b_skip: float32 [768], P('mp'), may hold values from -1.5 to 1.5
- gain_attn: float32 [768], P('mp'), may hold values from 0.1 to 1.9
- shift_attn: float32 [768], P('mp'), may hold values from -1.5 to 1.5
- w_qkv: bfloat16 [768, 3, 768], P('dp', None, 'mp'), may hold values from -0.21875 to 0.21875
- b_qv: float32 [2, 768], P(None, 'mp'), may hold values from -1.5 to 1.5
- w_out: bfloat16 [768, 768], P('mp', 'dp'), may hold values from -0.875 to 0.875
- b_out: float32 [768], P('mp'), may hold values from -1.5 to 1.5
- gain_mlp: float32 [768], P('mp'), may hold values from 0.1 to 1.9
- shift_mlp: float32 [768], P('mp'), may hold values from -1.5 to 1.5
- w_up: bfloat16 [768, 3072], P('dp', 'mp'), may hold values from -0.21875 to 0.21875
- b_up: float32 [3072], P('mp'), may hold values from -1.5 to 1.5
- w_down: bfloat16 [3072, 768], P('mp', 'dp'), may hold values from -0.15625 to 0.15625
- b_down: float32 [768], P('mp'), may hold values from -1.5 to 1.5
- cotangent: bfloat16 [12288, 768], P(('dp', 'mp')), may hold values from -6 to 6
Outputs:
- layer_out: bfloat16 [12288, 768], P(('dp', 'mp'))
- grad_tokens: float32 [12288, 768], P(('dp', 'mp'))
- grad_skip: float32 [12288, 768], P(('dp', 'mp'))
- grad_w_skip: float32 [1536, 768], P('dp', 'mp')
- grad_b_skip: float32 [768], P('mp')
- grad_gain_attn: float32 [768], P('mp')
- grad_shift_attn: float32 [768], P('mp')
- grad_w_qkv: float32 [768, 3, 768], P('dp', None, 'mp')
- grad_b_qv: float32 [2, 768], P(None, 'mp')
- grad_w_out: float32 [768, 768], P('mp', 'dp')
- grad_b_out: float32 [768], P('mp')
- grad_gain_mlp: float32 [768], P('mp')
- grad_shift_mlp: float32 [768], P('mp')
- grad_w_up: float32 [768, 3072], P('dp', 'mp')
- grad_b_up: float32 [3072], P('mp')
- grad_w_down: float32 [3072, 768], P('mp', 'dp')
- grad_b_down: float32 [768], P('mp')
The draws below stay inside these ranges and needn't reach their ends.
All inputs are finite; a program needn't handle non-finite values. No bound on the sum of `caption_flag` or of `caption_mask` on one device may be relied on, other than what follows from the above.
Results may differ from the reference program's by a relative error of at most 0.014.
Values may be sent and summed in bfloat16 or wider, within the bound.
A program may use at most 128 MiB of HBM per device.

```python
import math
import jax
import jax.numpy as jnp
from jax import lax

D = 768
HEADS = 12
FF = 3072
HEAD = 64
LAT = 257
CAP = 77
SLOT = 384
ITEMS_DEV = 4
ITEMS = 32
TOKENS = 12288
N_DP = 8


def place_ends(values, own_key, smallest, top_value):
    place = [jax.random.randint(jax.random.fold_in(own_key, axis), (), 0, length) for axis, length in enumerate(values.shape)]
    main_axis = values.shape.index(max(values.shape))
    beside = place[:main_axis] + [(place[main_axis] + 1) % values.shape[main_axis]] + place[main_axis + 1:]
    return values.at[tuple(place)].set(smallest).at[tuple(beside)].set(top_value)


def block_scale(key, dims, shards, least, top_value):
    def one(dim, shards_of):
        draws = jax.random.uniform(jax.random.fold_in(jax.random.fold_in(key, 6), dim), (shards_of,), jnp.float32, least / len(shards), top_value / len(shards))
        return jnp.repeat(jnp.exp(draws), dims[dim] // shards_of).reshape((-1,) + (1,) * (len(dims) - dim - 1))

    level = one(*shards[0])
    for cut in shards[1:]:
        level = level * one(*cut)
    return level


def centred(rng, extent, spread, reach, shards=(), kind=jnp.bfloat16):
    entries = jax.random.normal(rng, extent, jnp.float32) * spread
    if len(shards) > 0:
        entries = block_scale(rng, extent, shards, -0.22, 0.18) * entries
    return jnp.clip(entries, min=-reach, max=reach).astype(kind)


def setup_inputs(seed: int = 0) -> dict:
    keys = jax.random.split(jax.random.key(seed), 20)
    tokens_in = centred(keys[0], (TOKENS, D), 1.0, 6.0, ((0, 32),))
    skip_tokens = centred(keys[1], (TOKENS, D), 1.0, 6.0, ((0, 32),))
    caption_flag = place_ends((jax.random.randint(keys[2], (ITEMS,), 0, 2) < 1).astype(jnp.int32), jax.random.fold_in(keys[2], 1), 0, 1)
    caption_mask = place_ends((jax.random.randint(keys[3], (ITEMS, CAP), 0, 4) < 3).astype(jnp.int32), jax.random.fold_in(keys[3], 1), 0, 1)
    w_skip = centred(keys[4], (2 * D, D), (2 * D) ** -0.5, 0.15625, ((0, 8), (1, 4)))
    b_skip = centred(keys[5], (D,), 0.3, 1.5, ((0, 4),), jnp.float32)
    gain_attn = jnp.clip(1.0 + 0.18 * jax.random.normal(keys[6], (D,), jnp.float32), 0.1, 1.9)
    shift_attn = centred(keys[7], (D,), 0.3, 1.5, ((0, 4),), jnp.float32)
    w_qkv = centred(keys[8], (D, 3, D), D ** -0.5, 0.21875, ((0, 8), (2, 4)))
    b_qv = centred(keys[9], (2, D), 0.3, 1.5, ((1, 4),), jnp.float32)
    w_out = centred(keys[10], (D, D), (D // 16) ** -0.5, 0.875, ((0, 4), (1, 8)))
    b_out = centred(keys[11], (D,), 0.3, 1.5, ((0, 4),), jnp.float32)
    gain_mlp = jnp.clip(1.0 + 0.18 * jax.random.normal(keys[12], (D,), jnp.float32), 0.1, 1.9)
    shift_mlp = centred(keys[13], (D,), 0.3, 1.5, ((0, 4),), jnp.float32)
    w_up = centred(keys[14], (D, FF), D ** -0.5, 0.21875, ((0, 8), (1, 4)))
    b_up = centred(keys[15], (FF,), 0.3, 1.5, ((0, 4),), jnp.float32)
    w_down = centred(keys[16], (FF, D), (FF // 2) ** -0.5, 0.15625, ((0, 4), (1, 8)))
    b_down = centred(keys[17], (D,), 0.3, 1.5, ((0, 4),), jnp.float32)
    cotangent = centred(keys[18], (TOKENS, D), 1.0, 6.0, ((0, 32),))
    return dict(tokens_in=tokens_in, skip_tokens=skip_tokens, caption_flag=caption_flag, caption_mask=caption_mask, w_skip=w_skip, b_skip=b_skip, gain_attn=gain_attn, shift_attn=shift_attn, w_qkv=w_qkv, b_qv=b_qv, w_out=w_out, b_out=b_out, gain_mlp=gain_mlp, shift_mlp=shift_mlp, w_up=w_up, b_up=b_up, w_down=w_down, b_down=b_down, cotangent=cotangent)


exact_mode = lax.Precision.HIGHEST
norm_eps = 1e-05

@jax.custom_vjp
def low(v):
    return lax.optimization_barrier(v.astype(jnp.bfloat16)).astype(jnp.float32)

@jax.custom_vjp
def low_back(v):
    return v

def low_keep(v):
    return (low(v), None)

def low_pass(kept, grad):
    return (grad,)

def back_keep(v):
    return (v, None)

def back_low(kept, grad):
    return (low(grad),)
low.defvjp(low_keep, low_pass)
low_back.defvjp(back_keep, back_low)

def layer_norm(hidden, norm_gain, norm_shift):
    row_mean = lax.optimization_barrier(jnp.mean(hidden, axis=-1, keepdims=True))
    row_var = lax.optimization_barrier(jnp.mean(hidden * hidden, axis=-1, keepdims=True)) - row_mean * row_mean
    return (hidden - row_mean) * lax.rsqrt(row_var + norm_eps) * norm_gain + norm_shift

def live_rows(caption_flag, caption_mask):
    item_count = caption_flag.shape[0]
    positions = jnp.arange(SLOT, dtype=jnp.int32)
    padded = jnp.concatenate([jnp.zeros((item_count, LAT), jnp.int32), caption_mask.astype(jnp.int32), jnp.zeros((item_count, SLOT - LAT - CAP), jnp.int32)], axis=1)
    return jnp.where(positions[None, :] < LAT, 1, caption_flag.astype(jnp.int32)[:, None] * padded).astype(jnp.int32)

def heads_view(array, item_count):
    return array.reshape(item_count, SLOT, HEADS, HEAD)

def block(params, tokens_in, skip_tokens, live_mask):
    w_skip, b_skip, gain_attn, shift_attn, w_qkv, b_qv, w_out, b_out, gain_mlp, shift_mlp, w_up, b_up, w_down, b_down = params
    item_count = live_mask.shape[0]
    joined = jnp.concatenate([tokens_in, skip_tokens], axis=1)
    stream_zero = low_back(jnp.dot(joined, w_skip, precision=exact_mode) + b_skip)
    normed_one = low(layer_norm(stream_zero, gain_attn, shift_attn))
    project = jnp.einsum('rd,dtc->rtc', normed_one, w_qkv, precision=exact_mode)
    query = low(low_back(project[:, 0] + b_qv[0]))
    key_rows = low(low_back(project[:, 1]))
    value_rows = low(low_back(project[:, 2] + b_qv[1]))
    scores = low_back(jnp.einsum('isha,itha->ihst', heads_view(query, item_count), heads_view(key_rows, item_count), precision=exact_mode) / math.sqrt(HEAD))
    key_keep = (live_mask > 0)[:, None, None, :]
    probs = jax.nn.softmax(jnp.where(key_keep, scores, -1e+30), axis=-1)
    context = jnp.einsum('ihst,itha->isha', low(probs), heads_view(value_rows, item_count), precision=exact_mode)
    context = low(low_back(context.reshape(item_count * SLOT, D)))
    stream_one = stream_zero + low_back(jnp.dot(context, w_out, precision=exact_mode) + b_out)
    normed_two = low(layer_norm(stream_one, gain_mlp, shift_mlp))
    pre_act = low_back(jnp.dot(normed_two, w_up, precision=exact_mode) + b_up)
    hidden_low = low(jax.nn.gelu(pre_act, approximate=False))
    stream_two = stream_one + low_back(jnp.dot(hidden_low, w_down, precision=exact_mode) + b_down)
    return stream_two * live_mask.reshape(-1, 1).astype(jnp.float32)

def reference(tokens_in, skip_tokens, caption_flag, caption_mask, w_skip, b_skip, gain_attn, shift_attn, w_qkv, b_qv, w_out, b_out, gain_mlp, shift_mlp, w_up, b_up, w_down, b_down, cotangent):
    params = tuple((a.astype(jnp.float32) for a in (w_skip, b_skip, gain_attn, shift_attn, w_qkv, b_qv, w_out, b_out, gain_mlp, shift_mlp, w_up, b_up, w_down, b_down)))
    row_count = ITEMS_DEV * SLOT
    token_blocks = tokens_in.astype(jnp.float32).reshape(N_DP, row_count, D)
    skip_blocks = skip_tokens.astype(jnp.float32).reshape(N_DP, row_count, D)
    live_blocks = live_rows(caption_flag, caption_mask).reshape(N_DP, ITEMS_DEV, SLOT)
    checked = jax.checkpoint(block)

    def forward(params_in, token_part, skip_part):

        def one_block(pieces):
            return checked(params_in, pieces[0], pieces[1], pieces[2])
        return lax.map(one_block, (token_part, skip_part, live_blocks))
    result, pull = jax.vjp(forward, params, token_blocks, skip_blocks)
    grads, grad_tokens, grad_skip = pull(cotangent.astype(jnp.float32).reshape(N_DP, row_count, D))
    return (result.reshape(TOKENS, D).astype(jnp.bfloat16), grad_tokens.reshape(TOKENS, D), grad_skip.reshape(TOKENS, D), grads[0], grads[1], grads[2], grads[3], grads[4], grads[5], grads[6], grads[7], grads[8], grads[9], grads[10], grads[11], grads[12], grads[13])
```

```python
import math

import jax
import jax.numpy as jnp
from jax import lax
from jax.sharding import PartitionSpec as P

HEAD = 64
LAT = 257
BF = jnp.bfloat16
F32 = jnp.float32

norm_eps = 1e-05
inv_root_two = 0.7071067811865476
inv_root_tau = 0.3989422804014327


def rows_t(a, b):
    return lax.dot_general(a, b, (((0,), (0,)), ((), ())), preferred_element_type=F32)


def cols_t(a, b):
    return lax.dot_general(a, b, (((1,), (1,)), ((), ())), preferred_element_type=F32)


def mm(a, b):
    return jnp.dot(a, b, preferred_element_type=F32)


def norm_forward(hidden, gain, shift):
    mean = jnp.mean(hidden, axis=1, keepdims=True)
    var = jnp.mean(hidden * hidden, axis=1, keepdims=True) - mean * mean
    inverse = lax.rsqrt(var + norm_eps)
    centred = (hidden - mean) * inverse
    return (centred * gain + shift).astype(BF), centred, inverse


def norm_backward(grad, centred, inverse, gain):
    scaled = grad * gain
    first = jnp.mean(scaled, axis=1, keepdims=True)
    second = jnp.mean(scaled * centred, axis=1, keepdims=True)
    out = inverse * (scaled - first - centred * second)
    return out, jnp.sum(grad * centred, axis=0), jnp.sum(grad, axis=0)


def item_compute(tokens, skip, cot, live, weights, small):
    w_skip, w_qkv, w_out_t, w_up, w_down_t = weights
    (b_skip, gain_attn, shift_attn, b_q, b_v, b_out, gain_mlp, shift_mlp, b_down, b_up) = small
    items, slot = live.shape
    rows, width = tokens.shape
    heads = width // HEAD
    scale = 1.0 / math.sqrt(HEAD)
    keep = (live > 0)[:, None, None, :]
    live_col = live.reshape(rows, 1).astype(F32)

    def split(a):
        return a.reshape(items, slot, heads, HEAD)

    joined = jnp.concatenate([tokens, skip], axis=1)
    h0 = mm(joined, w_skip) + b_skip
    n1, xhat1, inv1 = norm_forward(h0, gain_attn, shift_attn)
    q = split((mm(n1, w_qkv[0]) + b_q).astype(BF))
    k = split(mm(n1, w_qkv[1]).astype(BF))
    v = split((mm(n1, w_qkv[2]) + b_v).astype(BF))
    scores = jnp.einsum("isha,itha->ihst", q, k, preferred_element_type=F32) * scale
    scores = jnp.where(keep, scores, -1e30)
    top = jnp.max(scores, axis=-1, keepdims=True)
    weight = jnp.exp(scores - top)
    probs = weight / jnp.sum(weight, axis=-1, keepdims=True)
    probs_low = probs.astype(BF)
    ctx = jnp.einsum("ihst,itha->isha", probs_low, v, preferred_element_type=F32)
    ctx = ctx.astype(BF).reshape(rows, width)
    h1 = h0 + cols_t(ctx, w_out_t) + b_out
    n2, xhat2, inv2 = norm_forward(h1, gain_mlp, shift_mlp)
    pre = mm(n2, w_up) + b_up
    cdf = 0.5 * (1.0 + lax.erf(pre * inv_root_two))
    pdf = jnp.exp(-0.5 * pre * pre) * inv_root_tau
    hid = (pre * cdf).astype(BF)
    h2 = h1 + cols_t(hid, w_down_t) + b_down
    layer_out = (h2 * live_col).astype(BF)

    dy_low = cot * live_col.astype(BF)
    dy = dy_low.astype(F32)
    g_b_down = jnp.sum(dy, axis=0)
    g_w_down_t = rows_t(dy_low, hid)
    dhid = mm(dy_low, w_down_t)
    dpre = (dhid * (cdf + pre * pdf)).astype(BF)
    g_b_up = jnp.sum(dpre.astype(F32), axis=0)
    g_w_up = rows_t(n2, dpre)
    dn2 = cols_t(dpre, w_up)
    back2, g_gain_mlp, g_shift_mlp = norm_backward(dn2, xhat2, inv2, gain_mlp)
    dh1 = dy + back2
    dattn = dh1.astype(BF)
    g_b_out = jnp.sum(dattn.astype(F32), axis=0)
    g_w_out_t = rows_t(dattn, ctx)
    dctx = split(mm(dattn, w_out_t).astype(BF))
    dprobs = jnp.einsum("isha,itha->ihst", dctx, v, preferred_element_type=F32)
    dot = jnp.sum(dprobs * probs, axis=-1, keepdims=True)
    dscore = (probs * (dprobs - dot)).astype(BF)
    dq = (jnp.einsum("ihst,itha->isha", dscore, k, preferred_element_type=F32) * scale).astype(BF)
    dk = (jnp.einsum("ihst,isha->itha", dscore, q, preferred_element_type=F32) * scale).astype(BF)
    dv = jnp.einsum("ihst,isha->itha", probs_low, dctx, preferred_element_type=F32).astype(BF)
    dq, dk, dv = (a.reshape(rows, width) for a in (dq, dk, dv))
    g_b_q = jnp.sum(dq.astype(F32), axis=0)
    g_b_v = jnp.sum(dv.astype(F32), axis=0)
    g_w_qkv = (rows_t(n1, dq), rows_t(n1, dk), rows_t(n1, dv))
    dn1 = cols_t(dq, w_qkv[0]) + cols_t(dk, w_qkv[1]) + cols_t(dv, w_qkv[2])
    back1, g_gain_attn, g_shift_attn = norm_backward(dn1, xhat1, inv1, gain_attn)
    dh0 = (dh1 + back1).astype(BF)
    g_b_skip = jnp.sum(dh0.astype(F32), axis=0)
    g_w_skip = rows_t(joined, dh0)
    g_tokens = cols_t(dh0, w_skip[:width])
    g_skip = cols_t(dh0, w_skip[width:])
    return (
        layer_out,
        g_tokens,
        g_skip,
        (g_w_skip, g_w_qkv, g_w_out_t, g_w_up, g_w_down_t),
        (g_b_skip, g_gain_attn, g_shift_attn, g_b_q, g_b_v, g_b_out, g_gain_mlp, g_shift_mlp, g_b_down, g_b_up),
    )


def live_rows(caption_flag, caption_mask, slot):
    items, width = caption_mask.shape
    positions = jnp.arange(slot, dtype=jnp.int32)
    padded = jnp.concatenate(
        [
            jnp.zeros((items, LAT), jnp.int32),
            caption_mask,
            jnp.zeros((items, slot - LAT - width), jnp.int32),
        ],
        axis=1,
    )
    return jnp.where(positions[None, :] < LAT, 1, caption_flag[:, None] * padded)


def local(
    tokens_in,
    skip_tokens,
    caption_flag,
    caption_mask,
    w_skip,
    b_skip,
    gain_attn,
    shift_attn,
    w_qkv,
    b_qv,
    w_out,
    b_out,
    gain_mlp,
    shift_mlp,
    w_up,
    b_up,
    w_down,
    b_down,
    cotangent,
):
    n_dp, n_mp = lax.axis_size("dp"), lax.axis_size("mp")
    both = ("dp", "mp")
    column = lax.axis_index("mp")
    cols = b_skip.shape[0]
    items = caption_flag.shape[0] // n_mp
    slot = tokens_in.shape[0] // items
    live = live_rows(caption_flag, caption_mask, slot)
    live = lax.dynamic_slice_in_dim(live, column * items, items, 0)

    packed = jnp.stack(
        [b_skip, gain_attn, shift_attn, b_qv[0], b_qv[1], b_out, gain_mlp, shift_mlp, b_down]
        + [b_up.reshape(4, -1)[i] for i in range(4)]
    )
    packed = lax.all_gather(packed, "mp", axis=0)
    whole = packed[:, :9].transpose(1, 0, 2).reshape(9, -1)
    small = tuple(whole[i] for i in range(9)) + (packed[:, 9:].reshape(-1),)

    tiles = (w_skip, w_qkv.transpose(1, 0, 2), w_out.T, w_up, w_down.T)
    flat = jnp.concatenate([t.reshape(-1, 384) for t in tiles], axis=0)
    gathered = lax.all_gather(flat, both, axis=0)
    parts = []
    at = 0
    for t in tiles:
        count = t.size // 384
        part = gathered[:, at : at + count].reshape((n_dp, n_mp) + t.shape)
        at += count
        if t.ndim == 2:
            part = part.transpose(0, 2, 1, 3).reshape(n_dp * t.shape[0], n_mp * t.shape[1])
        else:
            part = part.transpose(2, 0, 3, 1, 4).reshape(t.shape[0], n_dp * t.shape[1], n_mp * t.shape[2])
        parts.append(part)

    layer_out, g_tokens, g_skip, big, little = item_compute(
        tokens_in, skip_tokens, cotangent, live, tuple(parts), small
    )

    big = (big[0], jnp.stack([b.astype(BF) for b in big[1]]), big[2], big[3], big[4])
    pieces = []
    for g, t in zip(big, tiles):
        g = g.astype(BF)
        if t.ndim == 2:
            g = g.reshape(n_dp, t.shape[0], n_mp, t.shape[1]).transpose(0, 2, 1, 3)
        else:
            g = g.reshape(t.shape[0], n_dp, t.shape[1], n_mp, t.shape[2]).transpose(1, 3, 0, 2, 4)
        pieces.append(g.reshape(n_dp * n_mp, -1, 384))
    sums = lax.psum_scatter(jnp.concatenate(pieces, axis=1), both, scatter_dimension=0, tiled=False)
    sums = sums.astype(F32)
    outs = []
    at = 0
    for t in tiles:
        count = t.size // 384
        outs.append(sums[at : at + count].reshape(t.shape))
        at += count

    little = jnp.concatenate(
        [jnp.stack(little[:9]).reshape(9, n_mp, cols).transpose(1, 0, 2), little[9].reshape(n_mp, 4, cols)], axis=1
    )
    little = lax.psum(little, both)
    little = lax.dynamic_slice_in_dim(little, column, 1, 0)[0]
    return (
        layer_out,
        g_tokens,
        g_skip,
        outs[0],
        little[0],
        little[1],
        little[2],
        outs[1].transpose(1, 0, 2),
        little[3:5],
        outs[2].T,
        little[5],
        little[6],
        little[7],
        outs[3],
        little[9:].reshape(-1),
        outs[4].T,
        little[8],
    )


def solution(mesh):
    in_specs = (
        P(("dp", "mp"), None),
        P(("dp", "mp"), None),
        P("dp"),
        P("dp", None),
        P("dp", "mp"),
        P("mp"),
        P("mp"),
        P("mp"),
        P("dp", None, "mp"),
        P(None, "mp"),
        P("mp", "dp"),
        P("mp"),
        P("mp"),
        P("mp"),
        P("dp", "mp"),
        P("mp"),
        P("mp", "dp"),
        P("mp"),
        P(("dp", "mp"), None),
    )
    out_specs = (
        P(("dp", "mp"), None),
        P(("dp", "mp"), None),
        P(("dp", "mp"), None),
        P("dp", "mp"),
        P("mp"),
        P("mp"),
        P("mp"),
        P("dp", None, "mp"),
        P(None, "mp"),
        P("mp", "dp"),
        P("mp"),
        P("mp"),
        P("mp"),
        P("dp", "mp"),
        P("mp"),
        P("mp", "dp"),
        P("mp"),
    )
    return jax.shard_map(local, mesh=mesh, in_specs=in_specs, out_specs=out_specs, check_vma=False)
```

```python
import functools
import math

import jax
import jax.numpy as jnp
from jax import lax
from jax.experimental import pallas as pl
from jax.experimental.pallas import tpu as pltpu
from jax.sharding import PartitionSpec as P

HEAD = 64
LAT = 257
BF = jnp.bfloat16
F32 = jnp.float32

norm_eps = 1e-05
inv_root_two = 0.7071067811865476
inv_root_tau = 0.3989422804014327


def rows_t(a, b):
    return lax.dot_general(a, b, (((0,), (0,)), ((), ())), preferred_element_type=F32)


def cols_t(a, b):
    return lax.dot_general(a, b, (((1,), (1,)), ((), ())), preferred_element_type=F32)


def mm(a, b):
    return jnp.dot(a, b, preferred_element_type=F32)


def norm_forward(hidden, gain, shift):
    mean = jnp.mean(hidden, axis=1, keepdims=True)
    var = jnp.mean(hidden * hidden, axis=1, keepdims=True) - mean * mean
    inverse = lax.rsqrt(var + norm_eps)
    centred = (hidden - mean) * inverse
    return (centred * gain + shift).astype(BF), centred, inverse


def norm_backward(grad, centred, inverse, gain):
    scaled = grad * gain
    first = jnp.mean(scaled, axis=1, keepdims=True)
    second = jnp.mean(scaled * centred, axis=1, keepdims=True)
    out = inverse * (scaled - first - centred * second)
    return out, jnp.sum(grad * centred, axis=0), jnp.sum(grad, axis=0)


def item_compute(tokens, skip, cot, live, weights, small):
    w_skip, w_qkv, w_out_t, w_up, w_down_t = weights
    (b_skip, gain_attn, shift_attn, b_q, b_v, b_out, gain_mlp, shift_mlp, b_down, b_up) = small
    items, slot = live.shape
    rows, width = tokens.shape
    heads = width // HEAD
    scale = 1.0 / math.sqrt(HEAD)
    keep = (live > 0)[:, None, None, :]
    live_col = live.reshape(rows, 1).astype(F32)

    def split(a):
        return a.reshape(items, slot, heads, HEAD)

    joined = jnp.concatenate([tokens, skip], axis=1)
    h0 = mm(joined, w_skip) + b_skip
    n1, xhat1, inv1 = norm_forward(h0, gain_attn, shift_attn)
    q = split((mm(n1, w_qkv[0]) + b_q).astype(BF))
    k = split(mm(n1, w_qkv[1]).astype(BF))
    v = split((mm(n1, w_qkv[2]) + b_v).astype(BF))
    scores = jnp.einsum("isha,itha->ihst", q, k, preferred_element_type=F32) * scale
    scores = jnp.where(keep, scores, -1e30)
    top = jnp.max(scores, axis=-1, keepdims=True)
    weight = jnp.exp(scores - top)
    probs = weight / jnp.sum(weight, axis=-1, keepdims=True)
    probs_low = probs.astype(BF)
    ctx = jnp.einsum("ihst,itha->isha", probs_low, v, preferred_element_type=F32)
    ctx = ctx.astype(BF).reshape(rows, width)
    h1 = h0 + cols_t(ctx, w_out_t) + b_out
    n2, xhat2, inv2 = norm_forward(h1, gain_mlp, shift_mlp)
    pre = mm(n2, w_up) + b_up
    cdf = 0.5 * (1.0 + lax.erf(pre * inv_root_two))
    pdf = jnp.exp(-0.5 * pre * pre) * inv_root_tau
    hid = (pre * cdf).astype(BF)
    h2 = h1 + cols_t(hid, w_down_t) + b_down
    layer_out = (h2 * live_col).astype(BF)

    dy_low = cot * live_col.astype(BF)
    dy = dy_low.astype(F32)
    g_b_down = jnp.sum(dy, axis=0)
    g_w_down_t = rows_t(dy_low, hid)
    dhid = mm(dy_low, w_down_t)
    dpre = (dhid * (cdf + pre * pdf)).astype(BF)
    g_b_up = jnp.sum(dpre.astype(F32), axis=0)
    g_w_up = rows_t(n2, dpre)
    dn2 = cols_t(dpre, w_up)
    back2, g_gain_mlp, g_shift_mlp = norm_backward(dn2, xhat2, inv2, gain_mlp)
    dh1 = dy + back2
    dattn = dh1.astype(BF)
    g_b_out = jnp.sum(dattn.astype(F32), axis=0)
    g_w_out_t = rows_t(dattn, ctx)
    dctx = split(mm(dattn, w_out_t).astype(BF))
    dprobs = jnp.einsum("isha,itha->ihst", dctx, v, preferred_element_type=F32)
    dot = jnp.sum(dprobs * probs, axis=-1, keepdims=True)
    dscore = (probs * (dprobs - dot)).astype(BF)
    dq = (jnp.einsum("ihst,itha->isha", dscore, k, preferred_element_type=F32) * scale).astype(BF)
    dk = (jnp.einsum("ihst,isha->itha", dscore, q, preferred_element_type=F32) * scale).astype(BF)
    dv = jnp.einsum("ihst,isha->itha", probs_low, dctx, preferred_element_type=F32).astype(BF)
    dq, dk, dv = (a.reshape(rows, width) for a in (dq, dk, dv))
    g_b_q = jnp.sum(dq.astype(F32), axis=0)
    g_b_v = jnp.sum(dv.astype(F32), axis=0)
    g_w_qkv = (rows_t(n1, dq), rows_t(n1, dk), rows_t(n1, dv))
    dn1 = cols_t(dq, w_qkv[0]) + cols_t(dk, w_qkv[1]) + cols_t(dv, w_qkv[2])
    back1, g_gain_attn, g_shift_attn = norm_backward(dn1, xhat1, inv1, gain_attn)
    dh0 = (dh1 + back1).astype(BF)
    g_b_skip = jnp.sum(dh0.astype(F32), axis=0)
    g_w_skip = rows_t(joined, dh0)
    g_tokens = cols_t(dh0, w_skip[:width])
    g_skip = cols_t(dh0, w_skip[width:])
    return (
        layer_out,
        g_tokens,
        g_skip,
        (g_w_skip, g_w_qkv, g_w_out_t, g_w_up, g_w_down_t),
        (g_b_skip, g_gain_attn, g_shift_attn, g_b_q, g_b_v, g_b_out, g_gain_mlp, g_shift_mlp, g_b_down, g_b_up),
    )


def live_rows(caption_flag, caption_mask, slot):
    items, width = caption_mask.shape
    positions = jnp.arange(slot, dtype=jnp.int32)
    padded = jnp.concatenate(
        [
            jnp.zeros((items, LAT), jnp.int32),
            caption_mask,
            jnp.zeros((items, slot - LAT - width), jnp.int32),
        ],
        axis=1,
    )
    return jnp.where(positions[None, :] < LAT, 1, caption_flag[:, None] * padded)


MESH = pl.DeviceIdType.MESH
LANES = 384
PIECES = 5


def piece_view(flavour, piece, arrays, dp, y, core):
    w_skip, w_qkv, w_out_t, w_up, w_down_t = arrays
    cols = pl.ds(pl.multiple_of(y * LANES, 128), LANES)
    if piece == 0:
        rows = w_skip.shape[0] // 8
        start = dp * rows + core * (rows // 2) + flavour * (rows // 4)
        return w_skip.at[pl.ds(pl.multiple_of(start, 16), rows // 4), cols]
    if piece in (1, 2):
        rows = w_out_t.shape[0] // 8
        span = pl.ds(pl.multiple_of(dp * rows + core * (rows // 2), 16), rows // 2)
        if flavour == 1 and piece == 2:
            return w_out_t.at[span, cols]
        return w_qkv.at[2 if flavour == 1 else piece - 1, span, cols]
    array = w_up if piece == 3 else w_down_t
    rows = array.shape[0] // 8
    start = y * (4 * LANES) + core * (2 * LANES) + flavour * LANES
    return array.at[pl.ds(pl.multiple_of(dp * rows, 16), rows), pl.ds(pl.multiple_of(start, 128), LANES)]


def own_view(flavour, piece, merged, up, down):
    half = merged.shape[0] // 6
    if piece == 0:
        return merged.at[pl.ds(flavour * half, half)]
    if piece in (1, 2):
        order = ((2, 3), (4, 5))[flavour]
        return merged.at[pl.ds(order[piece - 1] * half, half)]
    return (up if piece == 3 else down).at[:, pl.ds(flavour * LANES, LANES)]


def gather_kernel(
    narrow, up, down, little,
    w_skip, w_qkv, w_out_t, w_up, w_down_t, little_all,
    merged, other, own_sem, pair_sem, little_sem, z_sem, a_sem, b_sem, c_sem,
):
    dp, mp = lax.axis_index("dp"), lax.axis_index("mp")
    z, x, y, core = dp // 2, dp % 2, mp // 2, mp % 2
    arrays = (w_skip, w_qkv, w_out_t, w_up, w_down_t)

    def device(zz, xx, yy, cc):
        return (zz * 2 + xx, yy * 2 + cc)

    z_others = [(z + d) % 4 for d in (1, 2, 3)]
    partner = device(z, x, y, 1 - core)
    across = [device(z, x, 1 - y, core), device(z, x, 1 - y, 1 - core)]
    beside = device(z, 1 - x, y, core)
    barrier = pltpu.get_barrier_semaphore()
    friends = [device(zz, x, y, core) for zz in z_others] + [partner, beside] + across
    for friend in friends:
        pl.semaphore_signal(barrier, inc=1, device_id=friend, device_id_type=MESH)
    pl.semaphore_wait(barrier, len(friends))

    def remote(source, target, sems, index, to):
        return pltpu.make_async_remote_copy(
            src_ref=source,
            dst_ref=target,
            send_sem=sems.at[(0,) + index],
            recv_sem=sems.at[(1,) + index],
            device_id=to,
            device_id_type=MESH,
        )

    swap = remote(narrow.at[1 - core], other, pair_sem, (), partner)
    swap.start()
    pltpu.make_async_copy(little, little_all.at[mp], own_sem.at[2 * PIECES]).start()
    for i, to in enumerate([partner] + across):
        remote(little, little_all.at[mp], little_sem, (i,), to).start()

    def forward(flavour, piece, source, zz, xx, yy, stage):
        view = piece_view(flavour, piece, arrays, zz * 2 + xx, yy, core)
        source = view if source is None else source
        side = xx if flavour == 0 else yy
        if stage == 1:
            remote(source, view, a_sem, (flavour, piece, zz), (beside, across[0])[flavour]).start()
        if stage <= 2:
            remote(source, view, b_sem, (flavour, piece, side * 4 + zz), (across[0], beside)[flavour]).start()
        remote(source, view, c_sem, (flavour, piece, (xx * 2 + yy) * 4 + zz), partner).start()

    def start_own(flavour, piece):
        source = own_view(flavour, piece, merged, up, down)
        view = piece_view(flavour, piece, arrays, dp, y, core)
        pltpu.make_async_copy(source, view, own_sem.at[flavour * PIECES + piece]).start()
        for i, zz in enumerate(z_others):
            pltpu.make_async_remote_copy(
                src_ref=source, dst_ref=view,
                send_sem=z_sem.at[0, flavour, piece, i],
                recv_sem=z_sem.at[1, flavour, piece, z],
                device_id=device(zz, x, y, core), device_id_type=MESH,
            ).start()
        forward(flavour, piece, source, z, x, y, 1)

    def arrived(flavour, piece, zz, xx, yy, sems, index):
        view = piece_view(flavour, piece, arrays, zz * 2 + xx, yy, core)
        remote(view, view, sems, index, partner).wait_recv()

    remote(narrow.at[0], other, pair_sem, (), partner).wait_recv()
    mine, theirs = narrow[core], other[...]
    lead = jnp.where(core == 0, mine, theirs)
    tail = jnp.where(core == 0, theirs, mine)
    merged[...] = jnp.concatenate([lead, tail], axis=1)
    for piece in range(PIECES):
        for flavour in (0, 1):
            start_own(flavour, piece)

    def stage_z(piece):
        for flavour in (0, 1):
            for zz in z_others:
                arrived(flavour, piece, zz, x, y, z_sem, (flavour, piece, zz))
                forward(flavour, piece, None, zz, x, y, 1)

    def stage_a(piece):
        for zz in [z] + z_others:
            for flavour in (0, 1):
                xx, yy = ((1 - x, y), (x, 1 - y))[flavour]
                arrived(flavour, piece, zz, xx, yy, a_sem, (flavour, piece, zz))
                forward(flavour, piece, None, zz, xx, yy, 2)

    def stage_b(piece):
        for near in (0, 1):
            for zz in [z] + z_others:
                for flavour in (0, 1):
                    if flavour == 0:
                        xx, yy = (x if near == 0 else 1 - x), 1 - y
                        side = xx
                    else:
                        xx, yy = 1 - x, (y if near == 0 else 1 - y)
                        side = yy
                    arrived(flavour, piece, zz, xx, yy, b_sem, (flavour, piece, side * 4 + zz))
                    forward(flavour, piece, None, zz, xx, yy, 3)

    for step in range(PIECES + 2):
        if step < PIECES:
            stage_z(step)
        if 1 <= step <= PIECES:
            stage_a(step - 1)
        if step >= 2:
            stage_b(step - 2)

    swap.wait_send()
    pltpu.make_async_copy(little, little_all.at[mp], own_sem.at[2 * PIECES]).wait()
    for i, to in enumerate([partner] + across):
        copy = remote(little, little_all.at[0], little_sem, (i,), to)
        copy.wait_send()
        copy.wait_recv()
    for flavour in (0, 1):
        for piece in range(PIECES):
            view = piece_view(flavour, piece, arrays, dp, y, core)
            pltpu.make_async_copy(
                own_view(flavour, piece, merged, up, down), view, own_sem.at[flavour * PIECES + piece]
            ).wait()
            for i in range(3):
                remote(view, view, z_sem, (flavour, piece, i), partner).wait_send()
            for i in range(4):
                remote(view, view, a_sem, (flavour, piece, i), partner).wait_send()
            for i in range(8):
                remote(view, view, b_sem, (flavour, piece, i), partner).wait_send()
            for i in range(16):
                copy = remote(view, view, c_sem, (flavour, piece, i), partner)
                copy.wait_send()
                copy.wait_recv()


def gather_weights(w_skip, w_qkv, w_out, w_up, w_down, little):
    def halves(tile):
        return tile.reshape(2, tile.shape[0] // 2, tile.shape[1])

    width = w_qkv.shape[0] * 8
    narrow = jnp.concatenate(
        [halves(w_skip)] + [halves(w_qkv[:, t]) for t in range(3)] + [halves(w_out.T)], axis=1
    )
    hidden = w_up.shape[1] * 4
    dma = pltpu.SemaphoreType.DMA
    any_space = pl.BlockSpec(memory_space=pl.ANY)
    vmem = pl.BlockSpec(memory_space=pltpu.VMEM)
    shape = jax.ShapeDtypeStruct
    return pl.pallas_call(
        gather_kernel,
        out_shape=(
            shape((2 * width, width), BF),
            shape((3, width, width), BF),
            shape((width, width), BF),
            shape((width, hidden), BF),
            shape((width, hidden), BF),
            shape((4,) + little.shape, F32),
        ),
        in_specs=[vmem] * 4,
        out_specs=(any_space,) * 6,
        scratch_shapes=[
            pltpu.VMEM((narrow.shape[1], LANES), BF),
            pltpu.VMEM(narrow.shape[1:], BF),
            dma((2 * PIECES + 1,)),
            dma((2,)),
            dma((2, 3)),
            dma((2, 2, PIECES, 4)),
            dma((2, 2, PIECES, 4)),
            dma((2, 2, PIECES, 8)),
            dma((2, 2, PIECES, 16)),
        ],
        compiler_params=pltpu.CompilerParams(collective_id=0, has_side_effects=True),
        name="gather_weights",
    )(narrow, w_up, w_down.T, little)


def whole_tiles(tiles, n_dp, n_mp):
    flat = jnp.concatenate([t.reshape(-1, 384) for t in tiles], axis=0)
    gathered = lax.all_gather(flat, ("dp", "mp"), axis=0)
    parts = []
    at = 0
    for t in tiles:
        count = t.size // 384
        part = gathered[:, at : at + count].reshape((n_dp, n_mp) + t.shape)
        at += count
        if t.ndim == 2:
            part = part.transpose(0, 2, 1, 3).reshape(n_dp * t.shape[0], n_mp * t.shape[1])
        else:
            part = part.transpose(2, 0, 3, 1, 4).reshape(t.shape[0], n_dp * t.shape[1], n_mp * t.shape[2])
        parts.append(part)
    return parts


def local(
    tokens_in,
    skip_tokens,
    caption_flag,
    caption_mask,
    w_skip,
    b_skip,
    gain_attn,
    shift_attn,
    w_qkv,
    b_qv,
    w_out,
    b_out,
    gain_mlp,
    shift_mlp,
    w_up,
    b_up,
    w_down,
    b_down,
    cotangent,
):
    n_dp, n_mp = lax.axis_size("dp"), lax.axis_size("mp")
    both = ("dp", "mp")
    column = lax.axis_index("mp")
    cols = b_skip.shape[0]
    items = caption_flag.shape[0] // n_mp
    slot = tokens_in.shape[0] // items
    live = live_rows(caption_flag, caption_mask, slot)
    live = lax.dynamic_slice_in_dim(live, column * items, items, 0)

    packed = jnp.stack(
        [b_skip, gain_attn, shift_attn, b_qv[0], b_qv[1], b_out, gain_mlp, shift_mlp, b_down]
        + [b_up.reshape(4, -1)[i] for i in range(4)]
    )
    tiles = (w_skip, w_qkv.transpose(1, 0, 2), w_out.T, w_up, w_down.T)
    fast = (n_dp, n_mp, cols) == (8, 4, 192) and w_up.shape == (96, 768)
    if fast:
        padded = jnp.pad(packed, ((0, 3), (0, 64)))
        *parts, packed = gather_weights(w_skip, w_qkv, w_out, w_up, w_down, padded)
        packed = packed[:, :13, :cols]
    else:
        packed = lax.all_gather(packed, "mp", axis=0)
        parts = whole_tiles(tiles, n_dp, n_mp)
    whole = packed[:, :9].transpose(1, 0, 2).reshape(9, -1)
    small = tuple(whole[i] for i in range(9)) + (packed[:, 9:].reshape(-1),)

    layer_out, g_tokens, g_skip, big, little = item_compute(
        tokens_in, skip_tokens, cotangent, live, tuple(parts), small
    )

    big = (big[0], jnp.stack([b.astype(BF) for b in big[1]]), big[2], big[3], big[4])
    pieces = []
    for g, t in zip(big, tiles):
        g = g.astype(BF)
        if t.ndim == 2:
            g = g.reshape(n_dp, t.shape[0], n_mp, t.shape[1]).transpose(0, 2, 1, 3)
        else:
            g = g.reshape(t.shape[0], n_dp, t.shape[1], n_mp, t.shape[2]).transpose(1, 3, 0, 2, 4)
        pieces.append(g.reshape(n_dp * n_mp, -1, 384))
    sums = lax.psum_scatter(jnp.concatenate(pieces, axis=1), both, scatter_dimension=0, tiled=False)
    sums = sums.astype(F32)
    outs = []
    at = 0
    for t in tiles:
        count = t.size // 384
        outs.append(sums[at : at + count].reshape(t.shape))
        at += count

    little = jnp.concatenate(
        [jnp.stack(little[:9]).reshape(9, n_mp, cols).transpose(1, 0, 2), little[9].reshape(n_mp, 4, cols)], axis=1
    )
    little = lax.psum(little, both)
    little = lax.dynamic_slice_in_dim(little, column, 1, 0)[0]
    return (
        layer_out,
        g_tokens,
        g_skip,
        outs[0],
        little[0],
        little[1],
        little[2],
        outs[1].transpose(1, 0, 2),
        little[3:5],
        outs[2].T,
        little[5],
        little[6],
        little[7],
        outs[3],
        little[9:].reshape(-1),
        outs[4].T,
        little[8],
    )


def solution(mesh):
    in_specs = (
        P(("dp", "mp"), None),
        P(("dp", "mp"), None),
        P("dp"),
        P("dp", None),
        P("dp", "mp"),
        P("mp"),
        P("mp"),
        P("mp"),
        P("dp", None, "mp"),
        P(None, "mp"),
        P("mp", "dp"),
        P("mp"),
        P("mp"),
        P("mp"),
        P("dp", "mp"),
        P("mp"),
        P("mp", "dp"),
        P("mp"),
        P(("dp", "mp"), None),
    )
    out_specs = (
        P(("dp", "mp"), None),
        P(("dp", "mp"), None),
        P(("dp", "mp"), None),
        P("dp", "mp"),
        P("mp"),
        P("mp"),
        P("mp"),
        P("dp", None, "mp"),
        P(None, "mp"),
        P("mp", "dp"),
        P("mp"),
        P("mp"),
        P("mp"),
        P("dp", "mp"),
        P("mp"),
        P("mp", "dp"),
        P("mp"),
    )
    return jax.shard_map(local, mesh=mesh, in_specs=in_specs, out_specs=out_specs, check_vma=False)
```

```python
import functools
import math

import jax
import jax.numpy as jnp
from jax import lax
from jax.experimental import pallas as pl
from jax.experimental.pallas import tpu as pltpu
from jax.sharding import PartitionSpec as P

HEAD = 64
LAT = 257
BF = jnp.bfloat16
F32 = jnp.float32

norm_eps = 1e-05
inv_root_two = 0.7071067811865476
inv_root_tau = 0.3989422804014327


def rows_t(a, b):
    return lax.dot_general(a, b, (((0,), (0,)), ((), ())), preferred_element_type=F32)


def cols_t(a, b):
    return lax.dot_general(a, b, (((1,), (1,)), ((), ())), preferred_element_type=F32)


def mm(a, b):
    return jnp.dot(a, b, preferred_element_type=F32)


def norm_forward(hidden, gain, shift):
    mean = jnp.mean(hidden, axis=1, keepdims=True)
    var = jnp.mean(hidden * hidden, axis=1, keepdims=True) - mean * mean
    inverse = lax.rsqrt(var + norm_eps)
    centred = (hidden - mean) * inverse
    return (centred * gain + shift).astype(BF), centred, inverse


def norm_backward(grad, centred, inverse, gain):
    scaled = grad * gain
    first = jnp.mean(scaled, axis=1, keepdims=True)
    second = jnp.mean(scaled * centred, axis=1, keepdims=True)
    out = inverse * (scaled - first - centred * second)
    return out, jnp.sum(grad * centred, axis=0), jnp.sum(grad, axis=0)


def item_compute(tokens, skip, cot, live, weights, small):
    w_skip, w_qkv, w_out_t, w_up, w_down_t = weights
    (b_skip, gain_attn, shift_attn, b_q, b_v, b_out, gain_mlp, shift_mlp, b_down, b_up) = small
    items, slot = live.shape
    rows, width = tokens.shape
    heads = width // HEAD
    scale = 1.0 / math.sqrt(HEAD)
    keep = (live > 0)[:, None, None, :]
    live_col = live.reshape(rows, 1).astype(F32)

    def split(a):
        return a.reshape(items, slot, heads, HEAD)

    joined = jnp.concatenate([tokens, skip], axis=1)
    h0 = mm(joined, w_skip) + b_skip
    n1, xhat1, inv1 = norm_forward(h0, gain_attn, shift_attn)
    q = split((mm(n1, w_qkv[0]) + b_q).astype(BF))
    k = split(mm(n1, w_qkv[1]).astype(BF))
    v = split((mm(n1, w_qkv[2]) + b_v).astype(BF))
    scores = jnp.einsum("isha,itha->ihst", q, k, preferred_element_type=F32) * scale
    scores = jnp.where(keep, scores, -1e30)
    top = jnp.max(scores, axis=-1, keepdims=True)
    weight = jnp.exp(scores - top)
    probs = weight / jnp.sum(weight, axis=-1, keepdims=True)
    probs_low = probs.astype(BF)
    ctx = jnp.einsum("ihst,itha->isha", probs_low, v, preferred_element_type=F32)
    ctx = ctx.astype(BF).reshape(rows, width)
    h1 = h0 + cols_t(ctx, w_out_t) + b_out
    n2, xhat2, inv2 = norm_forward(h1, gain_mlp, shift_mlp)
    pre = mm(n2, w_up) + b_up
    cdf = 0.5 * (1.0 + lax.erf(pre * inv_root_two))
    pdf = jnp.exp(-0.5 * pre * pre) * inv_root_tau
    hid = (pre * cdf).astype(BF)
    h2 = h1 + cols_t(hid, w_down_t) + b_down
    layer_out = (h2 * live_col).astype(BF)

    dy_low = cot * live_col.astype(BF)
    dy = dy_low.astype(F32)
    g_b_down = jnp.sum(dy, axis=0)
    g_w_down_t = rows_t(dy_low, hid)
    dhid = mm(dy_low, w_down_t)
    dpre = (dhid * (cdf + pre * pdf)).astype(BF)
    g_b_up = jnp.sum(dpre.astype(F32), axis=0)
    g_w_up = rows_t(n2, dpre)
    dn2 = cols_t(dpre, w_up)
    back2, g_gain_mlp, g_shift_mlp = norm_backward(dn2, xhat2, inv2, gain_mlp)
    dh1 = dy + back2
    dattn = dh1.astype(BF)
    g_b_out = jnp.sum(dattn.astype(F32), axis=0)
    g_w_out_t = rows_t(dattn, ctx)
    dctx = split(mm(dattn, w_out_t).astype(BF))
    dprobs = jnp.einsum("isha,itha->ihst", dctx, v, preferred_element_type=F32)
    dot = jnp.sum(dprobs * probs, axis=-1, keepdims=True)
    dscore = (probs * (dprobs - dot)).astype(BF)
    dq = (jnp.einsum("ihst,itha->isha", dscore, k, preferred_element_type=F32) * scale).astype(BF)
    dk = (jnp.einsum("ihst,isha->itha", dscore, q, preferred_element_type=F32) * scale).astype(BF)
    dv = jnp.einsum("ihst,isha->itha", probs_low, dctx, preferred_element_type=F32).astype(BF)
    dq, dk, dv = (a.reshape(rows, width) for a in (dq, dk, dv))
    g_b_q = jnp.sum(dq.astype(F32), axis=0)
    g_b_v = jnp.sum(dv.astype(F32), axis=0)
    g_w_qkv = (rows_t(n1, dq), rows_t(n1, dk), rows_t(n1, dv))
    dn1 = cols_t(dq, w_qkv[0]) + cols_t(dk, w_qkv[1]) + cols_t(dv, w_qkv[2])
    back1, g_gain_attn, g_shift_attn = norm_backward(dn1, xhat1, inv1, gain_attn)
    dh0 = (dh1 + back1).astype(BF)
    g_b_skip = jnp.sum(dh0.astype(F32), axis=0)
    g_w_skip = rows_t(joined, dh0)
    g_tokens = cols_t(dh0, w_skip[:width])
    g_skip = cols_t(dh0, w_skip[width:])
    return (
        layer_out,
        g_tokens,
        g_skip,
        (g_w_skip, g_w_qkv, g_w_out_t, g_w_up, g_w_down_t),
        (g_b_skip, g_gain_attn, g_shift_attn, g_b_q, g_b_v, g_b_out, g_gain_mlp, g_shift_mlp, g_b_down, g_b_up),
    )


def live_rows(caption_flag, caption_mask, slot):
    items, width = caption_mask.shape
    positions = jnp.arange(slot, dtype=jnp.int32)
    padded = jnp.concatenate(
        [
            jnp.zeros((items, LAT), jnp.int32),
            caption_mask,
            jnp.zeros((items, slot - LAT - width), jnp.int32),
        ],
        axis=1,
    )
    return jnp.where(positions[None, :] < LAT, 1, caption_flag[:, None] * padded)


MESH = pl.DeviceIdType.MESH
LANES = 384
PIECES = 5


def piece_view(flavour, piece, arrays, dp, y, core):
    w_skip, w_qkv, w_out_t, w_up, w_down_t = arrays
    cols = pl.ds(pl.multiple_of(y * LANES, 128), LANES)
    if piece == 0:
        rows = w_skip.shape[0] // 8
        start = dp * rows + core * (rows // 2) + flavour * (rows // 4)
        return w_skip.at[pl.ds(pl.multiple_of(start, 16), rows // 4), cols]
    if piece in (1, 2):
        rows = w_out_t.shape[0] // 8
        span = pl.ds(pl.multiple_of(dp * rows + core * (rows // 2), 16), rows // 2)
        if flavour == 1 and piece == 2:
            return w_out_t.at[span, cols]
        return w_qkv.at[2 if flavour == 1 else piece - 1, span, cols]
    array = w_up if piece == 3 else w_down_t
    rows = array.shape[0] // 8
    start = y * (4 * LANES) + core * (2 * LANES) + flavour * LANES
    return array.at[pl.ds(pl.multiple_of(dp * rows, 16), rows), pl.ds(pl.multiple_of(start, 128), LANES)]


def own_view(flavour, piece, merged, up, down):
    half = merged.shape[0] // 6
    if piece == 0:
        return merged.at[pl.ds(flavour * half, half)]
    if piece in (1, 2):
        order = ((2, 3), (4, 5))[flavour]
        return merged.at[pl.ds(order[piece - 1] * half, half)]
    return (up if piece == 3 else down).at[:, pl.ds(flavour * LANES, LANES)]


def gather_kernel(
    narrow, up, down, little,
    w_skip, w_qkv, w_out_t, w_up, w_down_t, little_all,
    merged, other, own_sem, pair_sem, little_sem, z_sem, a_sem, b_sem, c_sem,
):
    dp, mp = lax.axis_index("dp"), lax.axis_index("mp")
    z, x, y, core = dp // 2, dp % 2, mp // 2, mp % 2
    arrays = (w_skip, w_qkv, w_out_t, w_up, w_down_t)

    def device(zz, xx, yy, cc):
        return (zz * 2 + xx, yy * 2 + cc)

    z_others = [(z + d) % 4 for d in (1, 2, 3)]
    partner = device(z, x, y, 1 - core)
    across = [device(z, x, 1 - y, core), device(z, x, 1 - y, 1 - core)]
    beside = device(z, 1 - x, y, core)
    barrier = pltpu.get_barrier_semaphore()
    friends = [device(zz, x, y, core) for zz in z_others] + [partner, beside] + across
    for friend in friends:
        pl.semaphore_signal(barrier, inc=1, device_id=friend, device_id_type=MESH)
    pl.semaphore_wait(barrier, len(friends))

    def remote(source, target, sems, index, to):
        return pltpu.make_async_remote_copy(
            src_ref=source,
            dst_ref=target,
            send_sem=sems.at[(0,) + index],
            recv_sem=sems.at[(1,) + index],
            device_id=to,
            device_id_type=MESH,
        )

    swap = remote(narrow.at[1 - core], other, pair_sem, (), partner)
    swap.start()
    pltpu.make_async_copy(little, little_all.at[mp], own_sem.at[2 * PIECES]).start()
    for i, to in enumerate([partner] + across):
        remote(little, little_all.at[mp], little_sem, (i,), to).start()

    def forward(flavour, piece, source, zz, xx, yy, stage):
        view = piece_view(flavour, piece, arrays, zz * 2 + xx, yy, core)
        source = view if source is None else source
        side = xx if flavour == 0 else yy
        if stage == 1:
            remote(source, view, a_sem, (flavour, piece, zz), (beside, across[0])[flavour]).start()
        if stage <= 2:
            remote(source, view, b_sem, (flavour, piece, side * 4 + zz), (across[0], beside)[flavour]).start()
        remote(source, view, c_sem, (flavour, piece, (xx * 2 + yy) * 4 + zz), partner).start()

    def start_own(flavour, piece):
        source = own_view(flavour, piece, merged, up, down)
        view = piece_view(flavour, piece, arrays, dp, y, core)
        pltpu.make_async_copy(source, view, own_sem.at[flavour * PIECES + piece]).start()
        for i, zz in enumerate(z_others):
            pltpu.make_async_remote_copy(
                src_ref=source, dst_ref=view,
                send_sem=z_sem.at[0, flavour, piece, i],
                recv_sem=z_sem.at[1, flavour, piece, z],
                device_id=device(zz, x, y, core), device_id_type=MESH,
            ).start()
        forward(flavour, piece, source, z, x, y, 1)

    def arrived(flavour, piece, zz, xx, yy, sems, index):
        view = piece_view(flavour, piece, arrays, zz * 2 + xx, yy, core)
        remote(view, view, sems, index, partner).wait_recv()

    remote(narrow.at[0], other, pair_sem, (), partner).wait_recv()
    mine, theirs = narrow[core], other[...]
    lead = jnp.where(core == 0, mine, theirs)
    tail = jnp.where(core == 0, theirs, mine)
    merged[...] = jnp.concatenate([lead, tail], axis=1)
    for piece in range(PIECES):
        for flavour in (0, 1):
            start_own(flavour, piece)

    def stage_z(piece):
        for flavour in (0, 1):
            for zz in z_others:
                arrived(flavour, piece, zz, x, y, z_sem, (flavour, piece, zz))
                forward(flavour, piece, None, zz, x, y, 1)

    def stage_a(piece):
        for zz in [z] + z_others:
            for flavour in (0, 1):
                xx, yy = ((1 - x, y), (x, 1 - y))[flavour]
                arrived(flavour, piece, zz, xx, yy, a_sem, (flavour, piece, zz))
                forward(flavour, piece, None, zz, xx, yy, 2)

    def stage_b(piece):
        for near in (0, 1):
            for zz in [z] + z_others:
                for flavour in (0, 1):
                    if flavour == 0:
                        xx, yy = (x if near == 0 else 1 - x), 1 - y
                        side = xx
                    else:
                        xx, yy = 1 - x, (y if near == 0 else 1 - y)
                        side = yy
                    arrived(flavour, piece, zz, xx, yy, b_sem, (flavour, piece, side * 4 + zz))
                    forward(flavour, piece, None, zz, xx, yy, 3)

    for step in range(PIECES + 2):
        if step < PIECES:
            stage_z(step)
        if 1 <= step <= PIECES:
            stage_a(step - 1)
        if step >= 2:
            stage_b(step - 2)

    swap.wait_send()
    pltpu.make_async_copy(little, little_all.at[mp], own_sem.at[2 * PIECES]).wait()
    for i, to in enumerate([partner] + across):
        copy = remote(little, little_all.at[0], little_sem, (i,), to)
        copy.wait_send()
        copy.wait_recv()
    for flavour in (0, 1):
        for piece in range(PIECES):
            view = piece_view(flavour, piece, arrays, dp, y, core)
            pltpu.make_async_copy(
                own_view(flavour, piece, merged, up, down), view, own_sem.at[flavour * PIECES + piece]
            ).wait()
            for i in range(3):
                remote(view, view, z_sem, (flavour, piece, i), partner).wait_send()
            for i in range(4):
                remote(view, view, a_sem, (flavour, piece, i), partner).wait_send()
            for i in range(8):
                remote(view, view, b_sem, (flavour, piece, i), partner).wait_send()
            for i in range(16):
                copy = remote(view, view, c_sem, (flavour, piece, i), partner)
                copy.wait_send()
                copy.wait_recv()


def gather_weights(w_skip, w_qkv, w_out, w_up, w_down, little):
    def halves(tile):
        return tile.reshape(2, tile.shape[0] // 2, tile.shape[1])

    width = w_qkv.shape[0] * 8
    narrow = jnp.concatenate(
        [halves(w_skip)] + [halves(w_qkv[:, t]) for t in range(3)] + [halves(w_out.T)], axis=1
    )
    hidden = w_up.shape[1] * 4
    dma = pltpu.SemaphoreType.DMA
    any_space = pl.BlockSpec(memory_space=pl.ANY)
    vmem = pl.BlockSpec(memory_space=pltpu.VMEM)
    shape = jax.ShapeDtypeStruct
    return pl.pallas_call(
        gather_kernel,
        out_shape=(
            shape((2 * width, width), BF),
            shape((3, width, width), BF),
            shape((width, width), BF),
            shape((width, hidden), BF),
            shape((width, hidden), BF),
            shape((4,) + little.shape, F32),
        ),
        in_specs=[vmem] * 4,
        out_specs=(any_space,) * 6,
        scratch_shapes=[
            pltpu.VMEM((narrow.shape[1], LANES), BF),
            pltpu.VMEM(narrow.shape[1:], BF),
            dma((2 * PIECES + 1,)),
            dma((2,)),
            dma((2, 3)),
            dma((2, 2, PIECES, 4)),
            dma((2, 2, PIECES, 4)),
            dma((2, 2, PIECES, 8)),
            dma((2, 2, PIECES, 16)),
        ],
        compiler_params=pltpu.CompilerParams(collective_id=0, has_side_effects=True),
        name="gather_weights",
    )(narrow, w_up, w_down.T, little)


ROW_AT = (0, 48, 96, 144, 240)
ROW_COUNT = (48, 48, 48, 96, 96)
ROWS = 336


def scatter_kernel(
    g_skip, g_qkv, g_out_t, g_up, g_down_t, little,
    narrow_out, up_out, down_out, little_out,
    own, from_core, from_b, from_a, from_z, final, outgoing, l_mp, l_send, l_x, l_z,
    own_sem, c_sem, b_sem, a_sem, z_sem, pair_sem, l_sem,
):
    dp, mp = lax.axis_index("dp"), lax.axis_index("mp")
    z, x, y, core = dp // 2, dp % 2, mp // 2, mp % 2
    arrays = (g_skip, g_qkv, g_out_t, g_up, g_down_t)

    def device(zz, xx, yy, cc):
        return (zz * 2 + xx, yy * 2 + cc)

    z_others = [(z + d) % 4 for d in (1, 2, 3)]
    partner = device(z, x, y, 1 - core)
    across = [device(z, x, 1 - y, core), device(z, x, 1 - y, 1 - core)]
    beside = device(z, 1 - x, y, core)
    barrier = pltpu.get_barrier_semaphore()
    friends = [device(zz, x, y, core) for zz in z_others] + [partner, beside] + across
    for friend in friends:
        pl.semaphore_signal(barrier, inc=1, device_id=friend, device_id_type=MESH)
    pl.semaphore_wait(barrier, len(friends))

    def remote(source, target, sems, send, recv, to):
        return pltpu.make_async_remote_copy(
            src_ref=source,
            dst_ref=target,
            send_sem=sems.at[(0,) + send],
            recv_sem=sems.at[(1,) + recv],
            device_id=to,
            device_id_type=MESH,
        )

    def span(piece):
        return pl.ds(ROW_AT[piece], ROW_COUNT[piece])

    def slot_of(zz, xx, yy):
        return (xx * 2 + yy) * 4 + zz

    def place(flavour, far_b, far_a):
        if flavour == 0:
            return (1 - x if far_a else x), (1 - y if far_b else y)
        return (1 - x if far_b else x), (1 - y if far_a else y)

    def loop(body, start=0):
        def step(d, carry):
            body((z + d) % 4)
            return carry

        lax.fori_loop(start, 4, step, 0)

    def core_copy(flavour, piece, zz, xx, yy):
        view = piece_view(flavour, piece, arrays, zz * 2 + xx, yy, 1 - core)
        slot = slot_of(zz, xx, yy)
        key = (flavour, piece, slot)
        return remote(view, from_core.at[flavour, slot, span(piece)], c_sem, key, key, partner)

    def own_copy(flavour, piece, zz, xx, yy):
        view = piece_view(flavour, piece, arrays, zz * 2 + xx, yy, core)
        slot = slot_of(zz, xx, yy)
        return pltpu.make_async_copy(view, own.at[flavour, slot, span(piece)], own_sem.at[flavour, piece, slot])

    kinds = ((1, 0), (1, 1), (0, 1), (0, 0))
    little_to = [partner] + across
    little_slot = [2 * y + 1 - core, 2 * (1 - y) + core, 2 * (1 - y) + 1 - core]

    def little_mp(i):
        return remote(little.at[little_slot[i]], l_mp.at[i], l_sem, (i,), (i,), little_to[i])

    for i in range(3):
        little_mp(i).start()
    for piece in range(PIECES):
        for far_b, far_a in kinds:
            for flavour in (0, 1):
                xx, yy = place(flavour, far_b, far_a)

                def begin(zz, flavour=flavour, xx=xx, yy=yy, piece=piece):
                    core_copy(flavour, piece, zz, xx, yy).start()
                    own_copy(flavour, piece, zz, xx, yy).start()

                loop(begin)

    def side_of(flavour, xx, yy):
        return xx if flavour == 0 else yy

    def base(flavour, piece, zz, xx, yy):
        core_copy(flavour, piece, zz, xx, yy).wait_recv()
        own_copy(flavour, piece, zz, xx, yy).wait()
        slot = slot_of(zz, xx, yy)
        return own[flavour, slot, span(piece)].astype(F32) + from_core[flavour, slot, span(piece)].astype(F32)

    def b_copy(flavour, piece, zz, xx, yy):
        slot = slot_of(zz, xx, yy)
        index = side_of(flavour, xx, yy) * 4 + zz
        key = (flavour, piece, index)
        to = across[0] if flavour == 0 else beside
        return remote(
            own.at[flavour, slot, span(piece)], from_b.at[flavour, index, span(piece)], b_sem, key, key, to
        )

    def a_copy(flavour, piece, zz, xx, yy):
        slot = slot_of(zz, xx, yy)
        key = (flavour, piece, zz)
        to = beside if flavour == 0 else across[0]
        return remote(own.at[flavour, slot, span(piece)], from_a.at[flavour, zz, span(piece)], a_sem, key, key, to)

    def z_copy(flavour, piece, zz):
        return remote(
            own.at[flavour, slot_of(zz, x, y), span(piece)],
            from_z.at[flavour, z, span(piece)],
            z_sem,
            (flavour, piece, zz),
            (flavour, piece, z),
            device(zz, x, y, core),
        )

    def z_arrival(flavour, piece, zz):
        target = from_z.at[flavour, zz, span(piece)]
        return remote(target, target, z_sem, (flavour, piece, zz), (flavour, piece, zz), partner)

    def with_b(flavour, piece, zz, xx, yy):
        total = base(flavour, piece, zz, xx, yy)
        b_copy(flavour, piece, zz, xx, yy).wait_recv()
        index = side_of(flavour, xx, yy) * 4 + zz
        return total + from_b[flavour, index, span(piece)].astype(F32)

    def with_a(flavour, piece, zz):
        total = with_b(flavour, piece, zz, x, y)
        a_copy(flavour, piece, zz, x, y).wait_recv()
        return total + from_a[flavour, zz, span(piece)].astype(F32)

    def keep(flavour, piece, zz, xx, yy, total):
        own[flavour, slot_of(zz, xx, yy), span(piece)] = total.astype(BF)

    def stage_b(piece):
        for far_a in (1, 0):
            def body(zz, far_a=far_a):
                for flavour in (0, 1):
                    xx, yy = place(flavour, 1, far_a)
                    keep(flavour, piece, zz, xx, yy, base(flavour, piece, zz, xx, yy))
                    b_copy(flavour, piece, zz, xx, yy).start()

            loop(body)

    def stage_a(piece):
        def body(zz):
            for flavour in (0, 1):
                xx, yy = place(flavour, 0, 1)
                keep(flavour, piece, zz, xx, yy, with_b(flavour, piece, zz, xx, yy))
                a_copy(flavour, piece, zz, xx, yy).start()

        loop(body)

    def stage_z(piece):
        def body(zz):
            for flavour in (0, 1):
                keep(flavour, piece, zz, x, y, with_a(flavour, piece, zz))
                z_copy(flavour, piece, zz).start()

        loop(body, 1)

    def stage_end(piece):
        for flavour in (0, 1):
            total = with_a(flavour, piece, z)
            for zz in z_others:
                z_arrival(flavour, piece, zz).wait_recv()
                total = total + from_z[flavour, zz, span(piece)].astype(F32)
            if piece < 3:
                at = flavour if piece == 0 else (1 + piece if flavour == 0 else 3 + piece)
                final[pl.ds(48 * at, 48)] = total
            else:
                (up_out if piece == 3 else down_out)[:, pl.ds(LANES * flavour, LANES)] = total

    swap = pltpu.make_async_remote_copy(
        src_ref=outgoing, dst_ref=narrow_out.at[core], send_sem=pair_sem.at[0], recv_sem=pair_sem.at[1],
        device_id=partner, device_id_type=MESH,
    )
    little_x = remote(l_send.at[0], l_x, l_sem, (3,), (3,), beside)

    def little_z(i):
        return remote(l_send.at[1], l_z.at[z], l_sem, (4 + i,), (4 + z,), device(z_others[i], x, y, core))

    def little_z_in(zz):
        return remote(l_z.at[zz], l_z.at[zz], l_sem, (4,), (4 + zz,), partner)

    order = (4, 3, 0, 1, 2)
    for step in range(PIECES + 3):
        if step < PIECES:
            stage_b(order[step])
        if 0 <= step - 1 < PIECES:
            stage_a(order[step - 1])
        if 0 <= step - 2 < PIECES:
            stage_z(order[step - 2])
        if 0 <= step - 3 < PIECES:
            stage_end(order[step - 3])
        if step == 1:
            total = little[mp]
            for i in range(3):
                little_mp(i).wait_recv()
                total = total + l_mp[i]
            l_send[0] = total
            little_x.start()
        if step == 2:
            little_x.wait_recv()
            l_send[1] = l_send[0] + l_x[...]
            for i in range(3):
                little_z(i).start()
    sums = final[...]
    low, high = sums[:, : LANES // 2], sums[:, LANES // 2 :]
    narrow_out[core] = jnp.where(core == 0, low, high)
    outgoing[...] = jnp.where(core == 0, high, low)
    swap.start()
    total = l_send[1]
    for zz in z_others:
        little_z_in(zz).wait_recv()
        total = total + l_z[zz]
    little_out[...] = total

    for i in range(3):
        little_mp(i).wait_send()
        little_z(i).wait_send()
    little_x.wait_send()
    for piece in range(PIECES):
        for flavour in (0, 1):
            def drain(zz, flavour=flavour, piece=piece):
                for far_b, far_a in kinds:
                    xx, yy = place(flavour, far_b, far_a)
                    core_copy(flavour, piece, zz, xx, yy).wait_send()
                for far_a in (0, 1):
                    xx, yy = place(flavour, 1, far_a)
                    b_copy(flavour, piece, zz, xx, yy).wait_send()
                xx, yy = place(flavour, 0, 1)
                a_copy(flavour, piece, zz, xx, yy).wait_send()

            loop(drain)
            loop(lambda zz, flavour=flavour, piece=piece: z_copy(flavour, piece, zz).wait_send(), 1)
    pltpu.make_async_remote_copy(
        src_ref=outgoing, dst_ref=narrow_out.at[1 - core], send_sem=pair_sem.at[0], recv_sem=pair_sem.at[1],
        device_id=partner, device_id_type=MESH,
    ).wait()


def scatter_grads(g_skip, g_qkv, g_out_t, g_up, g_down_t, little):
    dma = pltpu.SemaphoreType.DMA
    any_space = pl.BlockSpec(memory_space=pl.ANY)
    vmem = pl.BlockSpec(memory_space=pltpu.VMEM)
    shape = jax.ShapeDtypeStruct
    tile = little.shape[1:]
    narrow, up, down, small = pl.pallas_call(
        scatter_kernel,
        out_shape=(
            shape((2, 288, LANES // 2), F32),
            shape((96, 2 * LANES), F32),
            shape((96, 2 * LANES), F32),
            shape(tile, F32),
        ),
        in_specs=[any_space] * 5 + [vmem],
        out_specs=(vmem,) * 4,
        scratch_shapes=[
            pltpu.VMEM((2, 16, ROWS, LANES), BF),
            pltpu.VMEM((2, 16, ROWS, LANES), BF),
            pltpu.VMEM((2, 8, ROWS, LANES), BF),
            pltpu.VMEM((2, 4, ROWS, LANES), BF),
            pltpu.VMEM((2, 4, ROWS, LANES), BF),
            pltpu.VMEM((288, LANES), F32),
            pltpu.VMEM((288, LANES // 2), F32),
            pltpu.VMEM((3,) + tile, F32),
            pltpu.VMEM((2,) + tile, F32),
            pltpu.VMEM(tile, F32),
            pltpu.VMEM((4,) + tile, F32),
            dma((2, PIECES, 16)),
            dma((2, 2, PIECES, 16)),
            dma((2, 2, PIECES, 8)),
            dma((2, 2, PIECES, 4)),
            dma((2, 2, PIECES, 4)),
            dma((2,)),
            dma((2, 8)),
        ],
        compiler_params=pltpu.CompilerParams(collective_id=1, has_side_effects=True),
        name="scatter_grads",
    )(g_skip, g_qkv, g_out_t, g_up, g_down_t, little)
    skip = narrow[:, :96].reshape(192, 192)
    qkv = jnp.stack([narrow[:, 96 + 48 * t : 144 + 48 * t].reshape(96, 192) for t in range(3)])
    return (skip, qkv, narrow[:, 240:].reshape(96, 192), up, down), small


def whole_tiles(tiles, n_dp, n_mp):
    flat = jnp.concatenate([t.reshape(-1, 384) for t in tiles], axis=0)
    gathered = lax.all_gather(flat, ("dp", "mp"), axis=0)
    parts = []
    at = 0
    for t in tiles:
        count = t.size // 384
        part = gathered[:, at : at + count].reshape((n_dp, n_mp) + t.shape)
        at += count
        if t.ndim == 2:
            part = part.transpose(0, 2, 1, 3).reshape(n_dp * t.shape[0], n_mp * t.shape[1])
        else:
            part = part.transpose(2, 0, 3, 1, 4).reshape(t.shape[0], n_dp * t.shape[1], n_mp * t.shape[2])
        parts.append(part)
    return parts


def tile_sums(big, tiles, n_dp, n_mp):
    pieces = []
    for g, t in zip(big, tiles):
        if t.ndim == 2:
            g = g.reshape(n_dp, t.shape[0], n_mp, t.shape[1]).transpose(0, 2, 1, 3)
        else:
            g = g.reshape(t.shape[0], n_dp, t.shape[1], n_mp, t.shape[2]).transpose(1, 3, 0, 2, 4)
        pieces.append(g.reshape(n_dp * n_mp, -1, 384))
    sums = lax.psum_scatter(jnp.concatenate(pieces, axis=1), ("dp", "mp"), scatter_dimension=0, tiled=False)
    sums = sums.astype(F32)
    outs = []
    at = 0
    for t in tiles:
        count = t.size // 384
        outs.append(sums[at : at + count].reshape(t.shape))
        at += count
    return outs


def local(
    tokens_in,
    skip_tokens,
    caption_flag,
    caption_mask,
    w_skip,
    b_skip,
    gain_attn,
    shift_attn,
    w_qkv,
    b_qv,
    w_out,
    b_out,
    gain_mlp,
    shift_mlp,
    w_up,
    b_up,
    w_down,
    b_down,
    cotangent,
):
    n_dp, n_mp = lax.axis_size("dp"), lax.axis_size("mp")
    both = ("dp", "mp")
    column = lax.axis_index("mp")
    cols = b_skip.shape[0]
    items = caption_flag.shape[0] // n_mp
    slot = tokens_in.shape[0] // items
    live = live_rows(caption_flag, caption_mask, slot)
    live = lax.dynamic_slice_in_dim(live, column * items, items, 0)

    packed = jnp.stack(
        [b_skip, gain_attn, shift_attn, b_qv[0], b_qv[1], b_out, gain_mlp, shift_mlp, b_down]
        + [b_up.reshape(4, -1)[i] for i in range(4)]
    )
    tiles = (w_skip, w_qkv.transpose(1, 0, 2), w_out.T, w_up, w_down.T)
    fast = (n_dp, n_mp, cols) == (8, 4, 192) and w_up.shape == (96, 768)
    if fast:
        padded = jnp.pad(packed, ((0, 3), (0, 64)))
        *parts, packed = gather_weights(w_skip, w_qkv, w_out, w_up, w_down, padded)
        packed = packed[:, :13, :cols]
    else:
        packed = lax.all_gather(packed, "mp", axis=0)
        parts = whole_tiles(tiles, n_dp, n_mp)
    whole = packed[:, :9].transpose(1, 0, 2).reshape(9, -1)
    small = tuple(whole[i] for i in range(9)) + (packed[:, 9:].reshape(-1),)

    layer_out, g_tokens, g_skip, big, little = item_compute(
        tokens_in, skip_tokens, cotangent, live, tuple(parts), small
    )

    big = (big[0], jnp.stack([b.astype(BF) for b in big[1]]), big[2], big[3], big[4])
    big = tuple(g.astype(BF) for g in big)
    little = jnp.concatenate(
        [jnp.stack(little[:9]).reshape(9, n_mp, cols).transpose(1, 0, 2), little[9].reshape(n_mp, 4, cols)], axis=1
    )
    if fast:
        outs, little = scatter_grads(*big, jnp.pad(little, ((0, 0), (0, 3), (0, 64))))
        little = little[:13, :cols]
    else:
        outs = tile_sums(big, tiles, n_dp, n_mp)
        little = lax.psum(little, both)
        little = lax.dynamic_slice_in_dim(little, column, 1, 0)[0]
    return (
        layer_out,
        g_tokens,
        g_skip,
        outs[0],
        little[0],
        little[1],
        little[2],
        outs[1].transpose(1, 0, 2),
        little[3:5],
        outs[2].T,
        little[5],
        little[6],
        little[7],
        outs[3],
        little[9:].reshape(-1),
        outs[4].T,
        little[8],
    )


def solution(mesh):
    in_specs = (
        P(("dp", "mp"), None),
        P(("dp", "mp"), None),
        P("dp"),
        P("dp", None),
        P("dp", "mp"),
        P("mp"),
        P("mp"),
        P("mp"),
        P("dp", None, "mp"),
        P(None, "mp"),
        P("mp", "dp"),
        P("mp"),
        P("mp"),
        P("mp"),
        P("dp", "mp"),
        P("mp"),
        P("mp", "dp"),
        P("mp"),
        P(("dp", "mp"), None),
    )
    out_specs = (
        P(("dp", "mp"), None),
        P(("dp", "mp"), None),
        P(("dp", "mp"), None),
        P("dp", "mp"),
        P("mp"),
        P("mp"),
        P("mp"),
        P("dp", None, "mp"),
        P(None, "mp"),
        P("mp", "dp"),
        P("mp"),
        P("mp"),
        P("mp"),
        P("dp", "mp"),
        P("mp"),
        P("mp", "dp"),
        P("mp"),
    )
    return jax.shard_map(local, mesh=mesh, in_specs=in_specs, out_specs=out_specs, check_vma=False)
```
